256 devices in a mesh: dp: 8 (over x, core), tensor: 16 (over y, z_lo), pipe: 2 (over z_hi).
Axes of the slice: x: 4, y: 4, z: 8 (z_hi: 2, z_lo: 4; z = z_hi * 4 + z_lo), core: 2. Of those that a mesh axis runs over, the one named last changes fastest.
Arguments:
- hidden: bfloat16 [2, 1024, 7168], P('pipe', ('dp', 'tensor')), may hold values from -200 to 200
- head_table: bfloat16 [81920, 7168], P(('dp', 'tensor')), may hold values from -1 to 1
- targets: int32 [2, 1024], P('pipe', ('dp', 'tensor')), may hold values from 0 to 81919
Outputs:
- token_loss: float32 [2, 1024], P('pipe', ('dp', 'tensor'))
- mean_loss: float32 [], replicated
The draws below stay inside these ranges and needn't reach their ends.
All inputs are finite; a program needn't handle non-finite values.
Results may differ from the reference program's by a relative error of at most 0.0003.
Values may be sent and summed in bfloat16 or wider, within the bound.
A program may use at most 128 MiB of HBM per device.

```python
import math
import jax
import jax.numpy as jnp
from jax import lax

D = 7168
V = 81920
GROUP = 1024
MICRO = 2


def table_row(key, row_index):
    base_key = jax.random.fold_in(key, 7001)
    values = jax.random.normal(jax.random.fold_in(base_key, row_index), (D,), jnp.float32) / math.sqrt(D)
    limit = 6.0 / math.sqrt(D)
    return jnp.clip(values, -limit, limit).astype(jnp.bfloat16).astype(jnp.float32)


def draw_head_table(key, part):
    return jax.vmap(lambda row_index: table_row(key, row_index))(jnp.arange(V)).astype(jnp.bfloat16)


def draw_hidden(key, part):
    own_key = jax.random.fold_in(key, 7002)
    keys = jax.random.split(own_key, 3)
    group_count = MICRO
    group_rise = 3.0 ** (jnp.arange(group_count, dtype=jnp.float32) / max(group_count - 1, 1))
    base_values = jax.random.normal(keys[0], (group_count, GROUP, D), jnp.float32)
    row_scale = jnp.exp(jax.random.uniform(keys[2], (group_count, GROUP, 1), jnp.float32, 0.0, math.log(3.0)))
    states = base_values * 1.5 * row_scale * group_rise[:, None, None]
    return jnp.clip(states, -200.0, 200.0).astype(jnp.bfloat16)


def touch_ends(values, key, least, top_value):
    extent = values.shape
    place = [jax.random.randint(jax.random.fold_in(key, axis), (), 0, extent[axis]) for axis in range(len(extent))]
    values = values.at[tuple(place)].set(least)
    longest = extent.index(max(extent))
    place[longest] = (place[longest] + 1) % extent[longest]
    return values.at[tuple(place)].set(top_value)


def setup_inputs(seed: int = 0) -> dict:
    streams_of = jax.random.split(jax.random.key(seed), 4)
    return {
        "hidden": draw_hidden(jax.random.fold_in(streams_of[3], 71), 0),
        "head_table": draw_head_table(jax.random.fold_in(streams_of[3], 71), 0),
        "targets": touch_ends(jax.random.randint(streams_of[2], (MICRO, GROUP), 0, V), jax.random.fold_in(streams_of[2], 1), 0, V - 1).astype(jnp.int32),
    }


def block_losses(token_block, label_block, head_table):
    logits = lax.dot_general(token_block, head_table, (((1,), (1,)), ((), ())), preferred_element_type=jnp.float32)
    maxima = jnp.max(logits, axis=1)
    sums = jnp.sum(jnp.exp(logits - maxima[:, None]), axis=1)
    columns = lax.broadcasted_iota(jnp.int32, logits.shape, 1)
    picked = jnp.sum(jnp.where(columns == label_block.astype(jnp.int32)[:, None], logits, jnp.zeros_like(logits)), axis=1)
    return maxima + jnp.log(sums) - picked


def reference(hidden, head_table, targets):
    pipe_count, group_size, model_width = hidden.shape
    all_tokens = pipe_count * group_size
    block_rows = math.gcd(all_tokens, 128)
    flat_rows = hidden.reshape(all_tokens // block_rows, block_rows, model_width)
    flat_labels = targets.reshape(all_tokens // block_rows, block_rows)
    losses = lax.map(lambda block_pair: block_losses(block_pair[0], block_pair[1], head_table), (flat_rows, flat_labels))
    token_loss = losses.reshape(pipe_count, group_size)
    mean_loss = jnp.sum(token_loss) / all_tokens
    return token_loss, mean_loss
```

```python
import functools

import jax
import jax.numpy as jnp
from jax import lax
from jax.experimental import pallas as pl
from jax.experimental.pallas import tpu as pltpu
from jax.sharding import Mesh
from jax.sharding import PartitionSpec as P

MESH = pl.DeviceIdType.MESH
NX, NY, NZ = 4, 4, 8
TILE = 128
OWN_TOKENS = 8
ORDERS = ("xyz", "yzx", "zxy")
SLOT_OFFSET = (0, -1, 1, -2)
TABLE_CHUNKS = 10


def kernel(
    hidden, table, targets, loss_out, mean_out,
    tok, tab, acc, stat, stat_in, part, part_in,
    local_sem, table_send, table_recv, send_sem, recv_sem,
    stat_send, stat_recv, part_send, part_recv,
):
    depth = hidden.shape[2]
    rows = table.shape[0]
    width = tok.shape[4] // 3
    x, core, y = lax.axis_index("x"), lax.axis_index("core"), lax.axis_index("y")
    z_lo, pipe = lax.axis_index("z_lo"), lax.axis_index("pipe")
    z = pipe * 4 + z_lo
    sign = 1 - 2 * core
    me = {"x": x, "y": y, "z": z}
    size = {"x": NX, "y": NY, "z": NZ}

    def device(xx, cc, yy, zz):
        return (xx, cc, yy, lax.rem(zz, 4), lax.div(zz, 4))

    def moved(dim, steps):
        at = dict(me)
        at[dim] = lax.rem(me[dim] + steps * sign + size[dim], size[dim])
        return device(at["x"], core, at["y"], at["z"])

    sibling = device(x, 1 - core, y, z)

    own_hidden = pltpu.make_async_copy(
        hidden.at[0], tok.at[0, y, x, :, pl.ds(0, depth)], local_sem.at[0]
    )
    own_hidden.start()
    own_table = pltpu.make_async_copy(
        table, tab.at[core, :, pl.ds(0, depth)], local_sem.at[1]
    )
    own_table.start()

    eye = lax.broadcasted_iota(jnp.int32, (8, 8), 0) == lax.broadcasted_iota(jnp.int32, (8, 8), 1)
    ids = jnp.broadcast_to(targets[...].astype(jnp.float32), (8, 8))
    column = jnp.sum(jnp.where(eye, ids, 0.0), axis=1, keepdims=True).astype(jnp.int32)
    column = jnp.broadcast_to(column, (8, TILE))
    lane = lax.broadcasted_iota(jnp.int32, (8, TILE), 1)
    digits = jnp.where(
        lane == 0, column & 63,
        jnp.where(lane == 1, (column >> 6) & 63, jnp.where(lane == 2, column >> 12, 0)),
    )
    tok[0, y, x, :, pl.ds(depth, TILE)] = digits.astype(jnp.float32).astype(jnp.bfloat16)
    tab[:, :, pl.ds(depth, TILE)] = jnp.zeros((2, rows, TILE), jnp.bfloat16)

    barrier = pltpu.get_barrier_semaphore()
    for dim in "xyz":
        for steps in (1, -1):
            pl.semaphore_signal(barrier, inc=1, device_id=moved(dim, steps), device_id_type=MESH)
    pl.semaphore_signal(barrier, inc=1, device_id=sibling, device_id_type=MESH)
    pl.semaphore_wait(barrier, 7)
    own_hidden.wait()

    def slot_at(dim, slot):
        if dim == "z":
            return slot
        return lax.rem(me[dim] + SLOT_OFFSET[slot] * sign + 4, 4)

    def index(q, where):
        picks = [where[dim] for dim in "zyx"]
        return (*picks, slice(None), pl.ds(q * width, width))

    copies = {}
    counts = [0, 0, 0]

    def send(q, phase, kind, tag, where):
        dim = ORDERS[q][phase]
        before = 1 if kind == "R" else 0
        after = {"M": 1, "m": 2, "R": 3}[kind]
        source, target = dict(where), dict(where)
        source[dim] = slot_at(dim, before)
        target[dim] = slot_at(dim, after) if dim == "z" else source[dim]
        number = counts[q]
        counts[q] += 1
        copy = pltpu.make_async_remote_copy(
            src_ref=tok.at[index(q, source)],
            dst_ref=tok.at[index(q, target)],
            send_sem=send_sem.at[q, number],
            recv_sem=recv_sem.at[q, number],
            device_id=moved(dim, -1 if kind == "m" else 1),
            device_id_type=MESH,
        )
        copy.start()
        copies[q, phase, kind, tag] = copy

    def arrived(q, phase, kind, tag):
        copies[q, phase, kind, tag].wait_recv()

    chunk = rows // TABLE_CHUNKS
    table_copies = []

    def send_table():
        k = len(table_copies)
        if k == TABLE_CHUNKS:
            return
        copy = pltpu.make_async_remote_copy(
            src_ref=table.at[pl.ds(k * chunk, chunk), :],
            dst_ref=tab.at[core, pl.ds(k * chunk, chunk), pl.ds(0, depth)],
            send_sem=table_send.at[k],
            recv_sem=table_recv.at[k],
            device_id=sibling,
            device_id_type=MESH,
        )
        copy.start()
        table_copies.append(copy)

    def where_of(q, **slots):
        found = {}
        for name, dim in zip(("d1", "d2", "d3"), ORDERS[q]):
            slot = slots.get(name, 0)
            if slot is None:
                found[dim] = pl.ds(0, 4)
            elif isinstance(slot, tuple):
                found[dim] = pl.ds(*slot)
            else:
                found[dim] = slot_at(dim, slot)
        return found

    thirds = range(3)

    def phase1(q, kind):
        send(q, 0, kind, 0, where_of(q))

    def phase2(q, kind, j):
        send(q, 1, kind, j, where_of(q, d1=j))

    def phase3(q, kind, j):
        send(q, 2, kind, j, where_of(q, d1=None, d2=j))

    for q in thirds:
        phase1(q, "M")
        phase1(q, "m")
    for q in thirds:
        phase2(q, "M", 0)
        phase2(q, "m", 0)
    send_table()
    for q in thirds:
        arrived(q, 0, "M", 0)
        phase1(q, "R")
        phase2(q, "M", 1)
        phase2(q, "m", 1)
    for q in thirds:
        arrived(q, 0, "m", 0)
        phase2(q, "M", 2)
        phase2(q, "m", 2)
    send_table()
    for q in thirds:
        arrived(q, 1, "M", 0)
        phase2(q, "R", 0)
    for q in thirds:
        arrived(q, 0, "R", 0)
        phase2(q, "M", 3)
        phase2(q, "m", 3)
        phase3(q, "M", 0)
        phase3(q, "m", 0)
    send_table()
    for j in (1, 2):
        for q in thirds:
            arrived(q, 1, "M", j)
            phase2(q, "R", j)
        send_table()
    for q in thirds:
        arrived(q, 1, "M", 3)
        phase2(q, "R", 3)
        phase3(q, "M", 1)
        phase3(q, "m", 1)
    send_table()
    for q in thirds:
        for j in range(4):
            arrived(q, 1, "m", j)
        phase3(q, "M", 2)
        phase3(q, "m", 2)
    send_table()
    for q in thirds:
        arrived(q, 2, "M", 0)
        if q == 2:
            send(q, 2, "R", (0, 0), where_of(q, d1=(0, 2), d2=0))
        else:
            phase3(q, "R", 0)
    send_table()
    for q in thirds:
        for j in range(4):
            arrived(q, 1, "R", j)
        phase3(q, "M", 3)
        phase3(q, "m", 3)
    send_table()
    send_table()
    for j in (1, 2, 3):
        for q in thirds:
            arrived(q, 2, "M", j)
            if q == 2:
                send(q, 2, "R", (0, j), where_of(q, d1=(0, 2), d2=j))
            else:
                phase3(q, "R", j)
    for j in range(4):
        send(2, 2, "R", (1, j), where_of(2, d1=(2, 2), d2=j))
    for q in thirds:
        for j in range(4):
            arrived(q, 2, "m", j)
    own_table.wait()
    for copy in table_copies:
        copy.wait_recv()

    group = 2 * NX * NY * OWN_TOKENS

    def product(half, q):
        tokens = tok[pl.ds(2 * half, 2), :, :, :, pl.ds(q * width, width)].reshape(group, width)
        rows_of = tab[:, :, pl.ds(q * width, width)].reshape(2 * rows, width)
        return lax.dot_general(
            rows_of, tokens, (((1,), (1,)), ((), ())), preferred_element_type=jnp.float32
        )

    base = lax.rem(x * 0 + ((x * 2) * 4 + y) * 4 + z_lo, 4 * 2 * 4 * 4) * rows
    step_to_sibling = 16 * rows

    def statistics(half):
        logits = acc[...]
        top = jnp.max(logits, axis=0, keepdims=True)
        total = jnp.sum(jnp.exp(logits - top), axis=0, keepdims=True)
        coded = tok[pl.ds(2 * half, 2), :, :, :, pl.ds(depth, TILE)].reshape(group, TILE)
        place = lax.broadcasted_iota(jnp.int32, (8, TILE), 1)
        weights = jnp.where(
            place == 0, 1.0, jnp.where(place == 1, 64.0, jnp.where(place == 2, 4096.0, 0.0))
        ).astype(jnp.bfloat16)
        wanted = lax.dot_general(
            weights, coded, (((1,), (1,)), ((), ())), preferred_element_type=jnp.float32
        )[0:1].astype(jnp.int32)
        row = lax.broadcasted_iota(jnp.int32, (2 * rows, group), 0)
        entry = base + row + jnp.where(row >= rows, step_to_sibling - rows, 0)
        picked = jnp.sum(jnp.where(entry == wanted, logits, 0.0), axis=0, keepdims=True)
        spread = top + jnp.log(total)
        for k in range(2):
            lanes = slice(k * TILE, (k + 1) * TILE)
            stat[2 * half + k, 0:1, :] = spread[:, lanes]
            stat[2 * half + k, 1:2, :] = picked[:, lanes]

    mine = x * 4 + y

    def send_statistics(slot):
        owner_z = lax.rem(z + SLOT_OFFSET[slot] * sign + NZ, NZ)

        def one(k, carry):
            peer = lax.rem(mine + k, 16)
            pltpu.make_async_remote_copy(
                src_ref=stat.at[slot],
                dst_ref=stat_in.at[slot, mine],
                send_sem=stat_send.at[slot],
                recv_sem=stat_recv.at[slot],
                device_id=device(lax.div(peer, 4), core, lax.rem(peer, 4), owner_z),
                device_id_type=MESH,
            ).start()
            return carry

        lax.fori_loop(1 if slot == 0 else 0, 16, one, 0)
        if slot == 0:
            stat_in[0, mine] = stat[0]

    def wait_bytes(ref, semaphore):
        pltpu.make_async_copy(ref, ref, semaphore).wait()

    acc[...] = product(0, 0)
    arrived(1, 2, "R", 0)
    arrived(1, 2, "R", 1)
    acc[...] += product(0, 1)
    for j in range(4):
        arrived(2, 2, "R", (0, j))
    acc[...] += product(0, 2)
    statistics(0)
    send_statistics(0)
    send_statistics(1)
    for j in range(4):
        arrived(0, 2, "R", j)
    acc[...] = product(1, 0)
    arrived(1, 2, "R", 2)
    arrived(1, 2, "R", 3)
    acc[...] += product(1, 1)
    for j in range(4):
        arrived(2, 2, "R", (1, j))
    acc[...] += product(1, 2)
    statistics(1)
    send_statistics(2)
    send_statistics(3)

    for copy in copies.values():
        copy.wait_send()
    for copy in table_copies:
        copy.wait_send()
    for slot in range(4):
        count = pl.ds(0, 15 if slot == 0 else 16)
        wait_bytes(stat_in.at[slot, count], stat_send.at[slot])
        wait_bytes(stat_in.at[slot, count], stat_recv.at[slot])

    everyone = stat_in[...].reshape(64, 2, TILE)
    spreads, found = everyone[:, 0, :], everyone[:, 1, :]
    top = jnp.max(spreads, axis=0, keepdims=True)
    total = jnp.sum(jnp.exp(spreads - top), axis=0, keepdims=True)
    losses = top + jnp.log(total) - jnp.sum(found, axis=0, keepdims=True)
    part_sum = jnp.sum(losses, axis=1, keepdims=True)
    own = z * 2 + core
    part[...] = jnp.broadcast_to(part_sum, (1, TILE))
    part_in[own] = jnp.broadcast_to(part_sum, (1, TILE))

    first = (y * NX + x) * OWN_TOKENS
    shifted = pltpu.roll(jnp.broadcast_to(losses, (8, TILE)), lax.rem(TILE - first, TILE), 1)
    loss_out[...] = shifted[0:1, 0:OWN_TOKENS]

    def send_part(k, carry):
        peer = lax.rem(own + k, 2 * NZ)
        pltpu.make_async_remote_copy(
            src_ref=part,
            dst_ref=part_in.at[own],
            send_sem=part_send,
            recv_sem=part_recv,
            device_id=device(x, lax.rem(peer, 2), y, lax.div(peer, 2)),
            device_id_type=MESH,
        ).start()
        return carry

    lax.fori_loop(1, 2 * NZ, send_part, 0)
    wait_bytes(part_in.at[pl.ds(0, 2 * NZ - 1)], part_send)
    wait_bytes(part_in.at[pl.ds(0, 2 * NZ - 1)], part_recv)
    sums = jnp.sum(part_in[...].reshape(2 * NZ, TILE), axis=0, keepdims=True)
    mean_out[...] = sums[:, 0:1] / (2 * NZ * TILE)


def body(hidden, head_table, targets):
    depth, rows = hidden.shape[2], head_table.shape[0]
    dma = pltpu.SemaphoreType.DMA
    losses, mean = pl.pallas_call(
        kernel,
        out_shape=(
            jax.ShapeDtypeStruct((1, OWN_TOKENS), jnp.float32),
            jax.ShapeDtypeStruct((1, 1), jnp.float32),
        ),
        in_specs=[
            pl.BlockSpec(memory_space=pl.ANY),
            pl.BlockSpec(memory_space=pl.ANY),
            pl.BlockSpec(memory_space=pltpu.VMEM),
        ],
        out_specs=(
            pl.BlockSpec(memory_space=pltpu.VMEM),
            pl.BlockSpec(memory_space=pltpu.VMEM),
        ),
        scratch_shapes=[
            pltpu.VMEM((4, NY, NX, OWN_TOKENS, depth + TILE), jnp.bfloat16),
            pltpu.VMEM((2, rows, depth + TILE), jnp.bfloat16),
            pltpu.VMEM((2 * rows, 2 * NX * NY * OWN_TOKENS), jnp.float32),
            pltpu.VMEM((4, 2, TILE), jnp.float32),
            pltpu.VMEM((4, 16, 2, TILE), jnp.float32),
            pltpu.VMEM((1, TILE), jnp.float32),
            pltpu.VMEM((2 * NZ, 1, TILE), jnp.float32),
            dma((2,)),
            dma((TABLE_CHUNKS,)),
            dma((TABLE_CHUNKS,)),
            dma((3, 32)),
            dma((3, 32)),
            dma((4,)),
            dma((4,)),
            dma,
            dma,
        ],
        compiler_params=pltpu.CompilerParams(collective_id=0, has_side_effects=True),
        name="head_loss",
    )(hidden, head_table, targets)
    return losses, mean.reshape(())


def solution(mesh):
    split = Mesh(
        mesh.devices.reshape(NX, 2, NY, 4, 2),
        ("x", "core", "y", "z_lo", "pipe"),
    )
    shards = ("x", "core", "y", "z_lo")
    return jax.shard_map(
        body,
        mesh=split,
        in_specs=(P("pipe", shards, None), P(shards, None), P("pipe", shards)),
        out_specs=(P("pipe", shards), P()),
        check_vma=False,
    )
```
